32 devices in a mesh: group: 8 (over z, x), slot: 4 (over y, core).
Axes of the slice: x: 2, y: 2, z: 4, core: 2. Of those that a mesh axis runs over, the one named last changes fastest.
Arguments:
- rows_in: bfloat16 [16384, 768], P(('group', 'slot')), may hold values from -6 to 6
- cotangent: bfloat16 [16384, 2048], P(('group', 'slot')), may hold values from -6 to 6
- gate_prob: float32 [16384], P(('group', 'slot')), may hold values from 0.05 to 0.5
- row_counts: int32 [32], P(('group', 'slot')), may hold values from 1 to 512
- old_place: int32 [32, 1], replicated, may hold values from 0 to 7
- new_place: int32 [32, 1], replicated, may hold values from 0 to 7
- rows_next: bfloat16 [16384, 768], P(('group', 'slot')), may hold values from -6 to 6
- master: float32 [8, 768, 2048], P(None, 'slot', 'group'), may hold values from -0.21875 to 0.21875
- moment_one: bfloat16 [8, 768, 2048], P(None, 'slot', 'group'), may hold values from -18 to 18
- moment_two: bfloat16 [8, 768, 2048], P(None, 'slot', 'group'), may hold values from 0.049804688 to 2
Outputs:
- input_grad: bfloat16 [16384, 768], P(('group', 'slot'))
- gate_grad: float32 [16384], P(('group', 'slot'))
- new_master: float32 [8, 768, 2048], P(None, 'slot', 'group')
- new_first: bfloat16 [8, 768, 2048], P(None, 'slot', 'group')
- new_second: bfloat16 [8, 768, 2048], P(None, 'slot', 'group')
- next_out: bfloat16 [16384, 2048], P(('group', 'slot'))
The draws below stay inside these ranges and needn't reach their ends.
Inputs may be any that keep to these rules, and one draw needn't show every extreme that they name: `old_place`: every one of the 8 experts is held by at least one of the 32 slots. `new_place`: every one of the 8 experts is listed for at least one of the 32 slots.
All inputs are finite; a program needn't handle non-finite values.
Results may differ from the reference program's by a relative error of at most 0.004.
The reference program's roundings to bfloat16 on the way count: a program that leaves them out, or rounds other values in their place, can miss the bound.
Values may be sent and summed in bfloat16 or wider, within the bound.
No kernel may reach another device: no remote copies, remote signals or barrier semaphores. Data moves between devices by JAX's collectives and lax.ppermute only.
A program may use at most 128 MiB of HBM per device.

```python
import math
import jax
import jax.numpy as jnp
from jax import lax

FF = 768
D = 2048
ROWS = 512
SLOTS = 32
EXPERTS = 8


def touch_ends(array, own_key, low, largest):
    longest = array.shape.index(max(array.shape))
    spots = []
    for shift in (0, 1):
        where = [jax.random.randint(jax.random.fold_in(own_key, axis), (), 0, length) for axis, length in enumerate(array.shape)]
        where[longest] = (where[longest] + shift) % array.shape[longest]
        spots.append(tuple(where))
    return array.at[spots[0]].set(low).at[spots[1]].set(largest)


def shard_levels(rng, extent, shards, low, high):
    factor_of, own = 1.0, jax.random.fold_in(rng, 6)
    for position, parts in shards:
        heights = jnp.exp(jax.random.uniform(jax.random.fold_in(own, position), (parts,), jnp.float32, low / len(shards), high / len(shards)))
        factor_of = factor_of * jnp.repeat(heights, extent[position] // parts).reshape([-1 if axis == position else 1 for axis in range(len(extent))])
    return factor_of


def choose_distinct(key, rows, number_of, top, lift):
    sequence = jax.random.permutation(jax.random.fold_in(key, 1), number_of)
    favour = sequence
    for power in range(3):
        favour = favour * favour // number_of
    favour = favour * lift // number_of
    chance = jax.random.randint(jax.random.fold_in(key, 2), (rows, number_of), 0, 4096) + favour
    fixed_rows = jax.random.permutation(jax.random.fold_in(key, 3), rows)[jnp.arange(number_of) % rows]
    chance = jnp.where(jnp.arange(rows)[:, None] == fixed_rows[None, :], 1 << 14, chance)
    merit = chance * number_of + jnp.arange(number_of)
    return lax.top_k(merit.astype(jnp.int32), top)[1].astype(jnp.int32)


def normal_values(rng, dims, spread, limit, cuts=(), kind=jnp.bfloat16):
    drawn = spread * jax.random.normal(rng, dims, jnp.float32)
    if cuts:
        drawn = drawn * shard_levels(rng, dims, cuts, -0.22, 0.18)
    return jnp.clip(drawn, -limit, limit).astype(kind)


def setup_inputs(seed: int = 0) -> dict:
    splits = jax.random.split(jax.random.key(seed), 11)
    return {
        "rows_in": normal_values(splits[0], (SLOTS * ROWS, FF), 1.0, 6.0, ((0, 32),)),
        "cotangent": normal_values(splits[1], (SLOTS * ROWS, D), 1.0, 6.0, ((0, 32),)),
        "gate_prob": jnp.clip(0.05 + 0.45 * jax.random.uniform(splits[2], (SLOTS * ROWS,), jnp.float32) ** shard_levels(splits[2], (SLOTS * ROWS,), ((0, 32),), -0.2, 0.2), 0.05, 0.5),
        "row_counts": touch_ends(jax.random.randint(splits[3], (SLOTS,), 1, ROWS + 1), jax.random.fold_in(splits[3], 1), 1, ROWS).astype(jnp.int32),
        "old_place": choose_distinct(splits[4], SLOTS, EXPERTS, 1, 2048),
        "new_place": choose_distinct(splits[5], SLOTS, EXPERTS, 1, 2048),
        "rows_next": normal_values(splits[6], (SLOTS * ROWS, FF), 1.0, 6.0, ((0, 32),)),
        "master": normal_values(splits[7], (EXPERTS, FF, D), FF ** -0.5, 0.21875, ((1, 4), (2, 8)), jnp.float32),
        "moment_one": normal_values(splits[8], (EXPERTS, FF, D), 3.0, 18.0, ((1, 4), (2, 8))),
        "moment_two": jnp.clip(jnp.exp(math.log(2.0) - 3.6927934 * jax.random.uniform(splits[9], (EXPERTS, FF, D), jnp.float32) ** shard_levels(splits[9], (EXPERTS, FF, D), ((1, 4), (2, 8)), -0.2, 0.2)), 0.049804688, 2.0).astype(jnp.bfloat16),
    }


beta_one = 0.9
beta_two = 0.999
adam_eps = 1e-08
learn_rate = 0.006
fix_one = 0.9999734386011124
fix_two = 0.0952078528862904

def reference(rows_in, cotangent, gate_prob, row_counts, old_place, new_place, rows_next, master, moment_one, moment_two):
    slot_rows = rows_in.reshape(SLOTS, ROWS, FF)
    slot_cot = cotangent.reshape(SLOTS, ROWS, D)
    slot_gate = gate_prob.reshape(SLOTS, ROWS)
    slot_next = rows_next.reshape(SLOTS, ROWS, FF)
    positions = jnp.arange(ROWS, dtype=jnp.int32)

    def run_slot(grad_sum, slot_item):
        inputs, upstream, gate_values, live_count, expert = slot_item
        live_rows = (positions < live_count)[:, None]
        masked_in = jnp.where(live_rows, inputs, jnp.zeros_like(inputs))
        masked_out = jnp.where(live_rows, upstream, jnp.zeros_like(upstream))
        weight = master[expert].astype(jnp.bfloat16)
        back_prod = jnp.dot(masked_out, weight.T, preferred_element_type=jnp.float32)
        input_grad = (gate_values[:, None] * back_prod).astype(jnp.bfloat16)
        forward_out = jnp.dot(masked_in, weight, preferred_element_type=jnp.float32)
        gate_grad = lax.optimization_barrier(jnp.sum(masked_out.astype(jnp.float32) * forward_out, axis=1))
        scaled_out = (gate_values[:, None] * masked_out.astype(jnp.float32)).astype(jnp.bfloat16)
        slot_grad = jnp.dot(masked_in.T, scaled_out, preferred_element_type=jnp.float32).astype(jnp.bfloat16)
        grad_sum = grad_sum.at[expert].add(slot_grad.astype(jnp.float32))
        return (grad_sum, (input_grad, gate_grad))
    zero_grad = jnp.zeros(master.shape, jnp.float32)
    grad_sum, (input_grad, gate_grad) = lax.scan(run_slot, zero_grad, (slot_rows, slot_cot, slot_gate, row_counts, old_place[:, 0]))
    first_full = beta_one * moment_one.astype(jnp.float32) + (1.0 - beta_one) * grad_sum
    second_full = beta_two * moment_two.astype(jnp.float32) + (1.0 - beta_two) * grad_sum * grad_sum
    new_master = master - learn_rate * (first_full / fix_one) / (jnp.sqrt(second_full / fix_two) + adam_eps)

    def run_next(slot_item):
        next_rows, expert = slot_item
        weight = new_master[expert].astype(jnp.bfloat16)
        return jnp.dot(next_rows, weight, preferred_element_type=jnp.float32).astype(jnp.bfloat16)
    next_out = lax.map(run_next, (slot_next, new_place[:, 0]))
    return (input_grad.reshape(SLOTS * ROWS, FF), gate_grad.reshape(SLOTS * ROWS), new_master, first_full.astype(jnp.bfloat16), second_full.astype(jnp.bfloat16), next_out.reshape(SLOTS * ROWS, D))
```

```python
import functools

import jax
import jax.numpy as jnp
from jax import lax
from jax.experimental import pallas as pl
from jax.experimental.pallas import tpu as pltpu
from jax.sharding import PartitionSpec as P

beta_one = 0.9
beta_two = 0.999
adam_eps = 1e-08
learn_rate = 0.006
fix_one = 0.9999734386011124
fix_two = 0.0952078528862904

BOTH = ("group", "slot")


def column_of(row):
    return jnp.transpose(jnp.broadcast_to(row, (8, row.shape[1])))[:, :1]


def slot_grad_kernel(count_ref, rows_ref, cot_ref, gate_ref, out_ref, turned):
    rows = rows_ref.shape[0]
    live = lax.broadcasted_iota(jnp.int32, (rows, 1), 0) < count_ref[0]

    @pl.when(pl.program_id(0) == 0)
    def _():
        kept = jnp.where(live, rows_ref[...].astype(jnp.float32), 0.0)
        turned[...] = jnp.transpose(kept).astype(jnp.bfloat16)

    scaled = column_of(gate_ref[...]) * cot_ref[...].astype(jnp.float32)
    scaled = jnp.where(live, scaled, 0.0).astype(jnp.bfloat16)
    out_ref[0] = jnp.dot(turned[...], scaled, preferred_element_type=jnp.float32).astype(
        jnp.bfloat16
    )


def slot_grads(row_counts, rows_in, cotangent, gate_row, group_count):
    rows, ff = rows_in.shape
    cols = cotangent.shape[1] // group_count
    return pl.pallas_call(
        slot_grad_kernel,
        name="slot_grads",
        out_shape=jax.ShapeDtypeStruct((group_count, ff, cols), jnp.bfloat16),
        grid_spec=pltpu.PrefetchScalarGridSpec(
            num_scalar_prefetch=1,
            grid=(group_count,),
            in_specs=[
                pl.BlockSpec((rows, ff), lambda g, c: (0, 0)),
                pl.BlockSpec((rows, cols), lambda g, c: (0, g)),
                pl.BlockSpec((1, rows), lambda g, c: (0, 0)),
            ],
            out_specs=pl.BlockSpec((1, ff, cols), lambda g, c: (g, 0, 0)),
            scratch_shapes=[pltpu.VMEM((ff, rows), jnp.bfloat16)],
        ),
        compiler_params=pltpu.CompilerParams(dimension_semantics=("arbitrary",)),
    )(row_counts, rows_in, cotangent, gate_row)


def update_kernel(
    old_ref, new_ref, grads_ref, master_ref, one_ref, two_ref,
    master_out, one_out, two_out, send_ref, total, fresh,
):
    slots = grads_ref.shape[0]
    total[...] = jnp.zeros_like(total)

    def add(s, _):
        e = old_ref[s]
        total[e] = total[e] + grads_ref[s].astype(jnp.float32)
        return 0

    lax.fori_loop(0, slots, add, 0)
    grad = total[...]
    first = beta_one * one_ref[...].astype(jnp.float32) + (1.0 - beta_one) * grad
    second = beta_two * two_ref[...].astype(jnp.float32) + (1.0 - beta_two) * grad * grad
    master = master_ref[...] - learn_rate * (first / fix_one) / (
        jnp.sqrt(second / fix_two) + adam_eps
    )
    master_out[...] = master
    one_out[...] = first.astype(jnp.bfloat16)
    two_out[...] = second.astype(jnp.bfloat16)
    fresh[...] = master.astype(jnp.bfloat16)

    def pick(s, _):
        send_ref[s] = fresh[new_ref[s]]
        return 0

    lax.fori_loop(0, slots, pick, 0)


def update(old, new, grads, master, one, two):
    slots, rows, cols = grads.shape
    experts = master.shape[0]
    step = 16
    state = pl.BlockSpec((experts, step, cols), lambda i, a, b: (0, i, 0))
    wide = pl.BlockSpec((slots, step, cols), lambda i, a, b: (0, i, 0))
    return pl.pallas_call(
        update_kernel,
        name="update",
        out_shape=(
            jax.ShapeDtypeStruct(master.shape, jnp.float32),
            jax.ShapeDtypeStruct(master.shape, jnp.bfloat16),
            jax.ShapeDtypeStruct(master.shape, jnp.bfloat16),
            jax.ShapeDtypeStruct(grads.shape, jnp.bfloat16),
        ),
        grid_spec=pltpu.PrefetchScalarGridSpec(
            num_scalar_prefetch=2,
            grid=(rows // step,),
            in_specs=[wide, state, state, state],
            out_specs=[state, state, state, wide],
            scratch_shapes=[
                pltpu.VMEM((experts, step, cols), jnp.float32),
                pltpu.VMEM((experts, step, cols), jnp.bfloat16),
            ],
        ),
        compiler_params=pltpu.CompilerParams(dimension_semantics=("arbitrary",)),
    )(old, new, grads, master, one, two)


def next_kernel(rows_ref, weight_ref, out_ref):
    out_ref[...] = jnp.dot(
        rows_ref[...], weight_ref[0], preferred_element_type=jnp.float32
    ).astype(jnp.bfloat16)


def next_rows(rows_next, weight):
    groups, ff, cols = weight.shape
    rows = rows_next.shape[0]
    return pl.pallas_call(
        next_kernel,
        name="next_rows",
        out_shape=jax.ShapeDtypeStruct((rows, groups * cols), jnp.bfloat16),
        grid=(groups,),
        in_specs=[
            pl.BlockSpec((rows, ff), lambda g: (0, 0)),
            pl.BlockSpec((1, ff, cols), lambda g: (g, 0, 0)),
        ],
        out_specs=pl.BlockSpec((rows, cols), lambda g: (0, g)),
        compiler_params=pltpu.CompilerParams(dimension_semantics=("arbitrary",)),
    )(rows_next, weight)


def back_kernel(count_ref, rows_ref, cot_ref, gate_ref, weight_ref, grad_ref, gate_out, total):
    g = pl.program_id(0)
    rows = rows_ref.shape[0]
    part = lax.dot_general(
        cot_ref[...],
        weight_ref[0],
        (((1,), (1,)), ((), ())),
        preferred_element_type=jnp.float32,
    )

    @pl.when(g == 0)
    def _():
        total[...] = part

    @pl.when(g > 0)
    def _():
        total[...] += part

    @pl.when(g == pl.num_programs(0) - 1)
    def _():
        live = lax.broadcasted_iota(jnp.int32, (rows, 1), 0) < count_ref[0]
        back = jnp.where(live, total[...], 0.0)
        grad_ref[...] = (column_of(gate_ref[...]) * back).astype(jnp.bfloat16)
        summed = jnp.sum(rows_ref[...].astype(jnp.float32) * back, axis=1, keepdims=True)
        gate_out[...] = jnp.transpose(jnp.broadcast_to(summed, (rows, 128)))[:1]


def back(row_counts, rows_in, cotangent, gate_row, weight):
    groups, ff, cols = weight.shape
    rows = rows_in.shape[0]
    return pl.pallas_call(
        back_kernel,
        name="back",
        out_shape=(
            jax.ShapeDtypeStruct((rows, ff), jnp.bfloat16),
            jax.ShapeDtypeStruct((1, rows), jnp.float32),
        ),
        grid_spec=pltpu.PrefetchScalarGridSpec(
            num_scalar_prefetch=1,
            grid=(groups,),
            in_specs=[
                pl.BlockSpec((rows, ff), lambda g, c: (0, 0)),
                pl.BlockSpec((rows, cols), lambda g, c: (0, g)),
                pl.BlockSpec((1, rows), lambda g, c: (0, 0)),
                pl.BlockSpec((1, ff, cols), lambda g, c: (g, 0, 0)),
            ],
            out_specs=[
                pl.BlockSpec((rows, ff), lambda g, c: (0, 0)),
                pl.BlockSpec((1, rows), lambda g, c: (0, 0)),
            ],
            scratch_shapes=[pltpu.VMEM((rows, ff), jnp.float32)],
        ),
        compiler_params=pltpu.CompilerParams(dimension_semantics=("arbitrary",)),
    )(row_counts, rows_in, cotangent, gate_row, weight)


def exchange(blocks):
    return lax.all_to_all(blocks, BOTH, split_axis=0, concat_axis=0, tiled=True)


def shards(
    rows_in, cotangent, gate_prob, row_counts, old_place, new_place, rows_next,
    master, moment_one, moment_two,
):
    slot_count = lax.axis_size("slot")
    group_count = lax.axis_size("group")
    part_rows, part_cols = master.shape[1:]
    ff = slot_count * part_rows
    old, new = old_place[:, 0], new_place[:, 0]
    gate_row = gate_prob.reshape(1, -1)
    grads = slot_grads(row_counts, rows_in, cotangent, gate_row, group_count)
    arrived = exchange(grads.reshape(-1, part_rows, part_cols))
    held = exchange(master[old].astype(jnp.bfloat16))
    new_master, new_first, new_second, send = update(
        old, new, arrived, master, moment_one, moment_two
    )
    weight = held.reshape(group_count, ff, part_cols)
    input_grad, gate_grad = back(row_counts, rows_in, cotangent, gate_row, weight)
    weight_next = exchange(send).reshape(group_count, ff, part_cols)
    next_out = next_rows(rows_next, weight_next)
    return input_grad, gate_grad.reshape(-1), new_master, new_first, new_second, next_out


def solution(mesh):
    rows = P(BOTH, None)
    row = P(BOTH)
    state = P(None, "slot", "group")
    return jax.shard_map(
        shards,
        mesh=mesh,
        in_specs=(rows, rows, row, row, P(), P(), rows, state, state, state),
        out_specs=(rows, row, state, state, state, rows),
        check_vma=False,
    )
```

```python
import functools

import jax
import jax.numpy as jnp
from jax import lax
from jax.experimental import pallas as pl
from jax.experimental.pallas import tpu as pltpu
from jax.sharding import PartitionSpec as P

beta_one = 0.9
beta_two = 0.999
adam_eps = 1e-08
learn_rate = 0.006
fix_one = 0.9999734386011124
fix_two = 0.0952078528862904

BOTH = ("group", "slot")


def column_of(row):
    return jnp.transpose(jnp.broadcast_to(row, (8, row.shape[1])))[:, :1]


def slot_grad_kernel(count_ref, rows_ref, cot_ref, gate_ref, out_ref, turned):
    rows = rows_ref.shape[0]
    live = lax.broadcasted_iota(jnp.int32, (rows, 1), 0) < count_ref[0]

    @pl.when(pl.program_id(0) == 0)
    def _():
        kept = jnp.where(live, rows_ref[...].astype(jnp.float32), 0.0)
        turned[...] = jnp.transpose(kept).astype(jnp.bfloat16)

    scaled = column_of(gate_ref[...]) * cot_ref[...].astype(jnp.float32)
    scaled = jnp.where(live, scaled, 0.0).astype(jnp.bfloat16)
    cols = out_ref.shape[2]
    for i in range(out_ref.shape[0]):
        out_ref[i] = jnp.dot(
            turned[...],
            scaled[:, i * cols : (i + 1) * cols],
            preferred_element_type=jnp.float32,
        ).astype(jnp.bfloat16)


def slot_grads(row_counts, rows_in, cotangent, gate_row, group_count):
    rows, ff = rows_in.shape
    cols = cotangent.shape[1] // group_count
    return pl.pallas_call(
        slot_grad_kernel,
        name="slot_grads",
        out_shape=jax.ShapeDtypeStruct((group_count, ff, cols), jnp.bfloat16),
        grid_spec=pltpu.PrefetchScalarGridSpec(
            num_scalar_prefetch=1,
            grid=(group_count // 2,),
            in_specs=[
                pl.BlockSpec((rows, ff), lambda g, c: (0, 0)),
                pl.BlockSpec((rows, 2 * cols), lambda g, c: (0, g)),
                pl.BlockSpec((1, rows), lambda g, c: (0, 0)),
            ],
            out_specs=pl.BlockSpec((2, ff, cols), lambda g, c: (g, 0, 0)),
            scratch_shapes=[pltpu.VMEM((ff, rows), jnp.bfloat16)],
        ),
        compiler_params=pltpu.CompilerParams(dimension_semantics=("arbitrary",)),
    )(row_counts, rows_in, cotangent, gate_row)


def update_kernel(
    old_ref, new_ref, grads_ref, master_ref, one_ref, two_ref,
    master_out, one_out, two_out, send_ref, total, fresh,
):
    slots = grads_ref.shape[0]
    total[...] = jnp.zeros_like(total)

    def add(s, _):
        e = old_ref[s]
        total[e] = total[e] + grads_ref[s].astype(jnp.float32)
        return 0

    lax.fori_loop(0, slots, add, 0, unroll=8)
    grad = total[...]
    first = beta_one * one_ref[...].astype(jnp.float32) + (1.0 - beta_one) * grad
    second = beta_two * two_ref[...].astype(jnp.float32) + (1.0 - beta_two) * grad * grad
    master = master_ref[...] - (learn_rate / fix_one) * first / (
        jnp.sqrt(second * (1.0 / fix_two)) + adam_eps
    )
    master_out[...] = master
    one_out[...] = first.astype(jnp.bfloat16)
    two_out[...] = second.astype(jnp.bfloat16)
    fresh[...] = master.astype(jnp.bfloat16)

    def pick(s, _):
        send_ref[s] = fresh[new_ref[s]]
        return 0

    lax.fori_loop(0, slots, pick, 0, unroll=8)


def update(old, new, grads, master, one, two):
    slots, rows, cols = grads.shape
    experts = master.shape[0]
    step = max(d for d in (16, 32, 48) if rows % d == 0)
    state = pl.BlockSpec((experts, step, cols), lambda i, a, b: (0, i, 0))
    wide = pl.BlockSpec((slots, step, cols), lambda i, a, b: (0, i, 0))
    return pl.pallas_call(
        update_kernel,
        name="update",
        out_shape=(
            jax.ShapeDtypeStruct(master.shape, jnp.float32),
            jax.ShapeDtypeStruct(master.shape, jnp.bfloat16),
            jax.ShapeDtypeStruct(master.shape, jnp.bfloat16),
            jax.ShapeDtypeStruct(grads.shape, jnp.bfloat16),
        ),
        grid_spec=pltpu.PrefetchScalarGridSpec(
            num_scalar_prefetch=2,
            grid=(rows // step,),
            in_specs=[wide, state, state, state],
            out_specs=[state, state, state, wide],
            scratch_shapes=[
                pltpu.VMEM((experts, step, cols), jnp.float32),
                pltpu.VMEM((experts, step, cols), jnp.bfloat16),
            ],
        ),
        compiler_params=pltpu.CompilerParams(dimension_semantics=("arbitrary",)),
    )(old, new, grads, master, one, two)


def next_kernel(rows_ref, weight_ref, out_ref):
    cols = weight_ref.shape[2]
    for i in range(weight_ref.shape[0]):
        out_ref[:, i * cols : (i + 1) * cols] = jnp.dot(
            rows_ref[...], weight_ref[i], preferred_element_type=jnp.float32
        ).astype(jnp.bfloat16)


def next_rows(rows_next, weight):
    groups, ff, cols = weight.shape
    rows = rows_next.shape[0]
    return pl.pallas_call(
        next_kernel,
        name="next_rows",
        out_shape=jax.ShapeDtypeStruct((rows, groups * cols), jnp.bfloat16),
        grid=(groups // 2,),
        in_specs=[
            pl.BlockSpec((rows, ff), lambda g: (0, 0)),
            pl.BlockSpec((2, ff, cols), lambda g: (g, 0, 0)),
        ],
        out_specs=pl.BlockSpec((rows, 2 * cols), lambda g: (0, g)),
        compiler_params=pltpu.CompilerParams(dimension_semantics=("arbitrary",)),
    )(rows_next, weight)


def exchange(blocks):
    return lax.all_to_all(blocks, BOTH, split_axis=0, concat_axis=0, tiled=True)


def along_line(mine, line, across):
    low, high, lows, highs = mine, mine, [], []
    for turn in range(line - 1):
        ups = [(g, g + across) for g in range(turn * across, (line - 1) * across)]
        downs = [(g + across, g) for g in range((line - 1 - turn) * across)]
        low = lax.ppermute(low, "group", ups)
        high = lax.ppermute(high, "group", downs)
        lows.append(low)
        highs.append(high)
    return lows, highs


def pick_kernel(pairs, plane_ref, wanted_ref, *rest):
    count = sum(2 if p else 1 for p in pairs)
    blocks, outs, sems = rest[:count], rest[count:-1], rest[-1]
    for j, out in enumerate(outs):
        at = 0
        for i, reach in enumerate(pairs):
            if not reach:
                pltpu.make_async_copy(
                    blocks[at].at[wanted_ref[j]], out.at[i], sems.at[j]
                ).start()
                at += 1
                continue
            for side in range(2):

                @pl.when((plane_ref[0] >= reach) == (side == 0))
                def _(block=blocks[at + side], out=out, i=i, j=j):
                    pltpu.make_async_copy(
                        block.at[wanted_ref[j]], out.at[i], sems.at[j]
                    ).start()

            at += 2
    for j, out in enumerate(outs):
        pltpu.make_async_copy(out, out, sems.at[j]).wait()


def picked(plane, wanted, entries):
    pairs = [entry[2] if len(entry) == 3 else 0 for entry in entries]
    blocks = [block for entry in entries for block in entry[:2]]
    piece = (len(entries),) + blocks[0].shape[1:]
    peers = wanted.shape[0]
    return pl.pallas_call(
        functools.partial(pick_kernel, pairs),
        name="picked",
        out_shape=[jax.ShapeDtypeStruct(piece, jnp.bfloat16)] * peers,
        in_specs=[pl.BlockSpec(memory_space=pltpu.SMEM)] * 2
        + [pl.BlockSpec(memory_space=pl.ANY)] * len(blocks),
        out_specs=[pl.BlockSpec(memory_space=pltpu.VMEM)] * peers,
        scratch_shapes=[pltpu.SemaphoreType.DMA((peers,))],
    )(plane, wanted, *blocks)


def among_peers(picks, peers, devices):
    parts = [picks[0]]
    for j in range(1, peers):
        pairs = [(p, p - p % peers + (p % peers ^ j)) for p in range(devices)]
        parts.append(lax.ppermute(picks[j], BOTH, pairs))
    return jnp.stack(parts)


def add_part(cot_ref, weights, total, first, valid):
    @pl.when(first)
    def _():
        total[...] = jnp.zeros_like(total)

    @pl.when(valid)
    def _():
        weight = jnp.concatenate([w[0, 0] for w in weights], axis=0)
        total[...] += lax.dot_general(
            cot_ref[...], weight, (((1,), (1,)), ((), ())), preferred_element_type=jnp.float32
        )


def near_kernel(across, me_ref, plane_ref, valid_ref, cot_ref, *rest):
    *weights, total = rest
    i = pl.program_id(0)
    add_part(cot_ref, weights, total, i == 0, valid_ref[i // across] == 1)


def far_kernel(
    across, me_ref, plane_ref, valid_ref, count_ref, cot_ref, rows_ref, gate_ref, so_far, *rest
):
    *weights, grad_ref, gate_out, total = rest
    i = pl.program_id(0)
    rows = rows_ref.shape[0]
    add_part(cot_ref, weights, total, i == 0, valid_ref[i // across] == 1)

    @pl.when(i == pl.num_programs(0) - 1)
    def _():
        live = lax.broadcasted_iota(jnp.int32, (rows, 1), 0) < count_ref[0]
        back = jnp.where(live, so_far[...] + total[...], 0.0)
        grad_ref[...] = (column_of(gate_ref[...]) * back).astype(jnp.bfloat16)
        summed = jnp.sum(rows_ref[...].astype(jnp.float32) * back, axis=1, keepdims=True)
        gate_out[...] = jnp.transpose(jnp.broadcast_to(summed, (rows, 128)))[:1]


def back_specs(parts, rows, across, slot_count):
    _, _, part_rows, cols = parts.shape

    def piece(k):
        def index(i, m, *_):
            return (((i % across) * slot_count + k) ^ m[0], i // across, 0, 0)

        return pl.BlockSpec((1, 1, part_rows, cols), index)

    def taken(i, m, plane, *_):
        return (0, plane[i // across] * across + i % across)

    return pl.BlockSpec((rows, cols), taken), [piece(k) for k in range(slot_count)]


def near_back(me, planes, valid, cotangent, parts, across, slot_count):
    rows, ff = cotangent.shape[0], slot_count * parts.shape[2]
    cot_spec, pieces = back_specs(parts, rows, across, slot_count)
    return pl.pallas_call(
        functools.partial(near_kernel, across),
        name="near_back",
        out_shape=jax.ShapeDtypeStruct((rows, ff), jnp.float32),
        grid_spec=pltpu.PrefetchScalarGridSpec(
            num_scalar_prefetch=3,
            grid=(parts.shape[1] * across,),
            in_specs=[cot_spec] + pieces,
            out_specs=pl.BlockSpec((rows, ff), lambda i, *_: (0, 0)),
        ),
        compiler_params=pltpu.CompilerParams(dimension_semantics=("arbitrary",)),
    )(me, planes, valid, cotangent, *([parts] * slot_count))


def far_back(
    me, planes, valid, row_counts, cotangent, rows_in, gate_row, so_far, parts, across, slot_count
):
    rows, ff = rows_in.shape
    cot_spec, pieces = back_specs(parts, rows, across, slot_count)
    whole = pl.BlockSpec((rows, ff), lambda i, *_: (0, 0))
    row = pl.BlockSpec((1, rows), lambda i, *_: (0, 0))
    return pl.pallas_call(
        functools.partial(far_kernel, across),
        name="far_back",
        out_shape=(
            jax.ShapeDtypeStruct((rows, ff), jnp.bfloat16),
            jax.ShapeDtypeStruct((1, rows), jnp.float32),
        ),
        grid_spec=pltpu.PrefetchScalarGridSpec(
            num_scalar_prefetch=4,
            grid=(parts.shape[1] * across,),
            in_specs=[cot_spec, whole, row, whole] + pieces,
            out_specs=[whole, row],
            scratch_shapes=[pltpu.VMEM((rows, ff), jnp.float32)],
        ),
        compiler_params=pltpu.CompilerParams(dimension_semantics=("arbitrary",)),
    )(
        me, planes, valid, row_counts, cotangent, rows_in, gate_row, so_far,
        *([parts] * slot_count),
    )


def shards(
    rows_in, cotangent, gate_prob, row_counts, old_place, new_place, rows_next,
    master, moment_one, moment_two,
):
    slot_count = lax.axis_size("slot")
    group_count = lax.axis_size("group")
    devices = group_count * slot_count
    _, part_rows, part_cols = master.shape
    ff = slot_count * part_rows
    across = 2
    line = group_count // across
    peers = across * slot_count
    g_own, k_own = lax.axis_index("group"), lax.axis_index("slot")
    plane = g_own // across
    me = (g_own % across) * slot_count + k_own
    old, new = old_place[:, 0], new_place[:, 0]
    gate_row = gate_prob.reshape(1, -1)

    mine = master.astype(jnp.bfloat16)
    lows, highs = along_line(mine, line, across)
    wanted = lax.dynamic_slice(old, (plane * peers,), (peers,))[
        me ^ jnp.arange(peers, dtype=jnp.int32)
    ]
    near, near_off, far, far_off = [(mine,)], [0], [], []
    for r in range(1, line):
        blocks, offs = (near, near_off) if r == 1 else (far, far_off)
        if 2 * r < line:
            blocks += [(lows[r - 1],), (highs[r - 1],)]
            offs += [-r, r]
        else:
            blocks.append((lows[r - 1], highs[r - 1], r))
            offs.append(jnp.where(plane >= r, -r, r))

    def table(offs):
        at = plane + jnp.stack([jnp.asarray(o, jnp.int32) for o in offs])
        valid = (at >= 0) & (at < line)
        return jnp.clip(at, 0, line - 1), valid.astype(jnp.int32)

    me_one, plane_one = me.reshape(1), plane.reshape(1)
    grads = slot_grads(row_counts, rows_in, cotangent, gate_row, group_count)
    arrived = exchange(grads.reshape(-1, part_rows, part_cols))
    parts = among_peers(picked(plane_one, wanted, near), peers, devices)
    so_far = near_back(me_one, *table(near_off), cotangent, parts, across, slot_count)

    new_master, new_first, new_second, send = update(
        old, new, arrived, master, moment_one, moment_two
    )
    weight_next = exchange(send).reshape(group_count, ff, part_cols)

    parts = among_peers(picked(plane_one, wanted, far), peers, devices)
    input_grad, gate_grad = far_back(
        me_one, *table(far_off), row_counts, cotangent, rows_in, gate_row, so_far, parts,
        across, slot_count,
    )
    next_out = next_rows(rows_next, weight_next)
    return input_grad, gate_grad.reshape(-1), new_master, new_first, new_second, next_out


def solution(mesh):
    rows = P(BOTH, None)
    row = P(BOTH)
    state = P(None, "slot", "group")
    return jax.shard_map(
        shards,
        mesh=mesh,
        in_specs=(rows, rows, row, row, P(), P(), rows, state, state, state),
        out_specs=(rows, row, state, state, state, rows),
        check_vma=False,
    )
```

```python
import functools

import jax
import jax.numpy as jnp
from jax import lax
from jax.experimental import pallas as pl
from jax.experimental.pallas import tpu as pltpu
from jax.sharding import Mesh
from jax.sharding import PartitionSpec as P

beta_one = 0.9
beta_two = 0.999
adam_eps = 1e-08
learn_rate = 0.006
fix_one = 0.9999734386011124
fix_two = 0.0952078528862904

WHOLE_VMEM = 67_000_000

LINE = ("half", "inner")
HALF = ("inner", "slot")
ALL = ("half", "inner", "slot")


def column_of(row):
    return jnp.transpose(jnp.broadcast_to(row, (8, row.shape[1])))[:, :1]


def slot_grad_kernel(count_ref, rows_ref, cot_ref, gate_ref, out_ref, turned):
    rows = rows_ref.shape[0]
    live = lax.broadcasted_iota(jnp.int32, (rows, 1), 0) < count_ref[0]

    @pl.when(pl.program_id(0) == 0)
    def _():
        kept = jnp.where(live, rows_ref[...].astype(jnp.float32), 0.0)
        turned[...] = jnp.transpose(kept).astype(jnp.bfloat16)

    scaled = column_of(gate_ref[...]) * cot_ref[...].astype(jnp.float32)
    scaled = jnp.where(live, scaled, 0.0).astype(jnp.bfloat16)
    cols = out_ref.shape[2]
    for i in range(out_ref.shape[0]):
        out_ref[i] = jnp.dot(
            turned[...],
            scaled[:, i * cols : (i + 1) * cols],
            preferred_element_type=jnp.float32,
        ).astype(jnp.bfloat16)


def slot_grads(row_counts, rows_in, cotangent, gate_row, group_count):
    rows, ff = rows_in.shape
    cols = cotangent.shape[1] // group_count
    return pl.pallas_call(
        slot_grad_kernel,
        name="slot_grads",
        out_shape=jax.ShapeDtypeStruct((group_count, ff, cols), jnp.bfloat16),
        grid_spec=pltpu.PrefetchScalarGridSpec(
            num_scalar_prefetch=1,
            grid=(group_count // 2,),
            in_specs=[
                pl.BlockSpec((rows, ff), lambda g, c: (0, 0)),
                pl.BlockSpec((rows, 2 * cols), lambda g, c: (0, g)),
                pl.BlockSpec((1, rows), lambda g, c: (0, 0)),
            ],
            out_specs=pl.BlockSpec((2, ff, cols), lambda g, c: (g, 0, 0)),
            scratch_shapes=[pltpu.VMEM((ff, rows), jnp.bfloat16)],
        ),
        compiler_params=pltpu.CompilerParams(
            dimension_semantics=("arbitrary",), vmem_limit_bytes=WHOLE_VMEM
        ),
    )(row_counts, rows_in, cotangent, gate_row)


def add_slots(place_ref, grads_ref, total):
    def add(s, _):
        e = place_ref[s]
        total[e] = total[e] + grads_ref[s].astype(jnp.float32)
        return 0

    lax.fori_loop(0, grads_ref.shape[0], add, 0, unroll=8)


def rows_step(rows):
    return max(d for d in (16, 32, 48) if rows % d == 0)


def update_kernel(
    old_ref, new_ref, grads_ref, master_ref, one_ref, two_ref,
    master_out, one_out, two_out, fresh_ref, send_ref, total,
):
    total[...] = jnp.zeros_like(total)
    add_slots(old_ref, grads_ref, total)
    grad = total[...]
    first = beta_one * one_ref[...].astype(jnp.float32) + (1.0 - beta_one) * grad
    second = beta_two * two_ref[...].astype(jnp.float32) + (1.0 - beta_two) * grad * grad
    master = master_ref[...] - (learn_rate / fix_one) * first / (
        jnp.sqrt(second * (1.0 / fix_two)) + adam_eps
    )
    master_out[...] = master
    one_out[...] = first.astype(jnp.bfloat16)
    two_out[...] = second.astype(jnp.bfloat16)
    fresh_ref[...] = master.astype(jnp.bfloat16)

    def pick(s, _):
        send_ref[s] = fresh_ref[new_ref[s]]
        return 0

    lax.fori_loop(0, send_ref.shape[0], pick, 0, unroll=8)


def update(old, new, grads, master, one, two):
    slots, rows, cols = grads.shape
    experts = master.shape[0]
    step = rows_step(rows)
    state = pl.BlockSpec((experts, step, cols), lambda i, a, b: (0, i, 0))
    wide = pl.BlockSpec((slots, step, cols), lambda i, a, b: (0, i, 0))
    near = pl.BlockSpec((new.shape[0], step, cols), lambda i, a, b: (0, i, 0))
    return pl.pallas_call(
        update_kernel,
        name="update",
        out_shape=(
            jax.ShapeDtypeStruct(master.shape, jnp.float32),
            jax.ShapeDtypeStruct(master.shape, jnp.bfloat16),
            jax.ShapeDtypeStruct(master.shape, jnp.bfloat16),
            jax.ShapeDtypeStruct(master.shape, jnp.bfloat16),
            jax.ShapeDtypeStruct(new.shape + (rows, cols), jnp.bfloat16),
        ),
        grid_spec=pltpu.PrefetchScalarGridSpec(
            num_scalar_prefetch=2,
            grid=(rows // step,),
            in_specs=[wide, state, state, state],
            out_specs=[state, state, state, state, near],
            scratch_shapes=[pltpu.VMEM((experts, step, cols), jnp.float32)],
        ),
        compiler_params=pltpu.CompilerParams(
            dimension_semantics=("arbitrary",), vmem_limit_bytes=WHOLE_VMEM
        ),
    )(old, new, grads, master, one, two)


def next_kernel(half_ref, rows_ref, weight_ref, *rest):
    out_ref = rest[-1]
    cols = weight_ref.shape[2]
    for i in range(2):
        out_ref[:, i * cols : (i + 1) * cols] = jnp.dot(
            rows_ref[...],
            weight_ref[2 * pl.program_id(0) + i],
            preferred_element_type=jnp.float32,
        ).astype(jnp.bfloat16)


def next_rows(half, rows_next, weight, so_far=None):
    inner, _, cols = weight.shape
    rows = rows_next.shape[0]
    pair = inner // 2
    more = () if so_far is None else (so_far,)
    return pl.pallas_call(
        next_kernel,
        name="next_rows",
        out_shape=jax.ShapeDtypeStruct((rows, 2 * inner * cols), jnp.bfloat16),
        grid_spec=pltpu.PrefetchScalarGridSpec(
            num_scalar_prefetch=1,
            grid=(pair,),
            in_specs=[pl.BlockSpec(memory_space=pltpu.VMEM)] * 2
            + [pl.BlockSpec(memory_space=pl.ANY)] * len(more),
            out_specs=pl.BlockSpec((rows, 2 * cols), lambda g, h: (0, h[0] * pair + g)),
        ),
        input_output_aliases={3: 0} if more else {},
        compiler_params=pltpu.CompilerParams(
            dimension_semantics=("arbitrary",), vmem_limit_bytes=WHOLE_VMEM
        ),
    )(half, rows_next, weight, *more)


def half_pick_kernel(wanted_ref, block_ref, out_ref):
    def pick(p, _):
        out_ref[p] = block_ref[wanted_ref[p]]
        return 0

    lax.fori_loop(0, out_ref.shape[0], pick, 0, unroll=4)


def half_picked(wanted, block):
    return pl.pallas_call(
        half_pick_kernel,
        name="half_picked",
        out_shape=jax.ShapeDtypeStruct(wanted.shape + block.shape[1:], jnp.bfloat16),
        in_specs=[
            pl.BlockSpec(memory_space=pltpu.SMEM),
            pl.BlockSpec(memory_space=pltpu.VMEM),
        ],
        out_specs=pl.BlockSpec(memory_space=pltpu.VMEM),
        compiler_params=pltpu.CompilerParams(vmem_limit_bytes=WHOLE_VMEM),
    )(wanted, block)


def along_line(mine, line, wide):
    low, high, lows, highs = mine, mine, [], []
    for turn in range(line - 1):
        ups = [(g, g + wide) for g in range(turn * wide, (line - 1) * wide)]
        downs = [(g + wide, g) for g in range((line - 1 - turn) * wide)]
        low = lax.ppermute(low, LINE, ups)
        high = lax.ppermute(high, LINE, downs)
        lows.append(low)
        highs.append(high)
    return lows, highs


def pick_kernel(pairs, plane_ref, wanted_ref, *rest):
    count = sum(2 if p else 1 for p in pairs)
    blocks, outs, sems = rest[:count], rest[count:-1], rest[-1]
    for j, out in enumerate(outs):
        at = 0
        for i, reach in enumerate(pairs):
            if not reach:
                pltpu.make_async_copy(
                    blocks[at].at[wanted_ref[j]], out.at[i], sems.at[j]
                ).start()
                at += 1
                continue
            for side in range(2):

                @pl.when((plane_ref[0] >= reach) == (side == 0))
                def _(block=blocks[at + side], out=out, i=i, j=j):
                    pltpu.make_async_copy(
                        block.at[wanted_ref[j]], out.at[i], sems.at[j]
                    ).start()

            at += 2
    for j, out in enumerate(outs):
        pltpu.make_async_copy(out, out, sems.at[j]).wait()


def picked(plane, wanted, entries, held=False):
    pairs = [entry[2] if len(entry) == 3 else 0 for entry in entries]
    blocks = [block for entry in entries for block in entry[:2]]
    piece = (len(entries),) + blocks[0].shape[1:]
    peers = wanted.shape[0]
    return pl.pallas_call(
        functools.partial(held_pick_kernel if held else pick_kernel, pairs),
        name="picked",
        out_shape=[jax.ShapeDtypeStruct(piece, jnp.bfloat16)] * peers,
        in_specs=[pl.BlockSpec(memory_space=pltpu.SMEM)] * 2
        + [pl.BlockSpec(memory_space=pltpu.VMEM if held else pl.ANY)] * len(blocks),
        out_specs=[pl.BlockSpec(memory_space=pltpu.VMEM)] * peers,
        scratch_shapes=[] if held else [pltpu.SemaphoreType.DMA((peers,))],
        compiler_params=pltpu.CompilerParams(vmem_limit_bytes=WHOLE_VMEM),
    )(plane, wanted, *blocks)


def held_pick_kernel(pairs, plane_ref, wanted_ref, *rest):
    count = sum(2 if p else 1 for p in pairs)
    blocks, outs = rest[:count], rest[count:]
    at = 0
    for i, reach in enumerate(pairs):
        if not reach:
            for j, out in enumerate(outs):
                out[i] = blocks[at][wanted_ref[j]]
            at += 1
            continue
        for side in range(2):

            @pl.when((plane_ref[0] >= reach) == (side == 0))
            def _(block=blocks[at + side], i=i):
                for j, out in enumerate(outs):
                    out[i] = block[wanted_ref[j]]

        at += 2


def among_peers(picks, peers, devices):
    parts = [picks[0]]
    for j in range(1, peers):
        pairs = [(p, p - p % peers + (p % peers ^ j)) for p in range(devices)]
        parts.append(lax.ppermute(picks[j], ALL, pairs))
    return parts


def back_kernel(wide, peers, slot_count, last, me_ref, plane_ref, valid_ref, *rest):
    parts, rest = rest[:peers], rest[peers:]
    cot_ref, rest = rest[0], rest[1:]
    if last:
        count_ref, rows_ref, gate_ref, so_far, grad_ref, gate_out, total, held, sems = rest
    elif len(rest) == 4:
        so_far, total, held, sems = rest
    else:
        so_far, (total, held, sems) = None, rest
    i = pl.program_id(0)

    @pl.when(i == 0)
    def _():
        copies = [pltpu.make_async_copy(part, held.at[j], sems.at[j]) for j, part in enumerate(parts)]
        for copy in copies:
            copy.start()
        total[...] = jnp.zeros_like(total) if so_far is None else so_far[...]
        for copy in copies:
            copy.wait()

    @pl.when(valid_ref[i // wide] == 1)
    def _():
        weight = jnp.concatenate(
            [
                held[((i % wide) * slot_count + k) ^ me_ref[0], i // wide]
                for k in range(slot_count)
            ],
            axis=0,
        )
        total[...] += lax.dot_general(
            cot_ref[...], weight, (((1,), (1,)), ((), ())), preferred_element_type=jnp.float32
        )

    if last:

        @pl.when(i == pl.num_programs(0) - 1)
        def _():
            rows = rows_ref.shape[0]
            live = lax.broadcasted_iota(jnp.int32, (rows, 1), 0) < count_ref[0]
            back = jnp.where(live, total[...], 0.0)
            grad_ref[...] = (column_of(gate_ref[...]) * back).astype(jnp.bfloat16)
            summed = jnp.sum(rows_ref[...].astype(jnp.float32) * back, axis=1, keepdims=True)
            gate_out[...] = jnp.transpose(jnp.broadcast_to(summed, (rows, 128)))[:1]


def back(me, planes, valid, cotangent, parts, wide, slot_count, so_far=None, last=None):
    peers = len(parts)
    entries, part_rows, cols = parts[0].shape
    rows, ff = cotangent.shape[0], slot_count * part_rows
    whole = pl.BlockSpec((rows, ff), lambda i, *_: (0, 0))
    row = pl.BlockSpec((1, rows), lambda i, *_: (0, 0))

    def taken(i, m, plane, *_):
        return (0, plane[i // wide] * wide + i % wide)

    total = jax.ShapeDtypeStruct((rows, ff), jnp.float32)
    specs = [pl.BlockSpec(memory_space=pl.ANY)] * peers + [pl.BlockSpec((rows, cols), taken)]
    scratch = [
        pltpu.VMEM((peers, entries, part_rows, cols), jnp.bfloat16),
        pltpu.SemaphoreType.DMA((peers,)),
    ]
    more = ()
    if last is not None:
        specs += [pl.BlockSpec(memory_space=pltpu.SMEM), whole, row]
        more = last
        total = (
            jax.ShapeDtypeStruct((rows, ff), jnp.bfloat16),
            jax.ShapeDtypeStruct((1, rows), jnp.float32),
        )
        scratch = [pltpu.VMEM((rows, ff), jnp.float32)] + scratch
    if so_far is not None:
        specs.append(whole)
        more += (so_far,)
    return pl.pallas_call(
        functools.partial(back_kernel, wide, peers, slot_count, last is not None),
        name="back",
        out_shape=total,
        grid_spec=pltpu.PrefetchScalarGridSpec(
            num_scalar_prefetch=3,
            grid=(entries * wide,),
            in_specs=specs,
            out_specs=whole if last is None else [whole, row],
            scratch_shapes=scratch,
        ),
        compiler_params=pltpu.CompilerParams(
            dimension_semantics=("arbitrary",), vmem_limit_bytes=WHOLE_VMEM
        ),
    )(me, planes, valid, *parts, cotangent, *more)


def exchange(blocks, axes):
    return lax.all_to_all(blocks, axes, split_axis=0, concat_axis=0, tiled=True)


def across(block):
    return lax.ppermute(block, "half", [(0, 1), (1, 0)])


def shards(
    rows_in, cotangent, gate_prob, row_counts, old_place, new_place, rows_next,
    master, moment_one, moment_two,
):
    inner, slot_count = lax.axis_size("inner"), lax.axis_size("slot")
    group_count, near_count = 2 * inner, inner * slot_count
    devices = group_count * slot_count
    _, part_rows, part_cols = master.shape
    ff = slot_count * part_rows
    wide = 2
    line = group_count // wide
    peers = wide * slot_count
    half = lax.axis_index("half")
    g_own, k_own = half * inner + lax.axis_index("inner"), lax.axis_index("slot")
    plane = g_own // wide
    me = (g_own % wide) * slot_count + k_own
    old = old_place[:, 0]
    new = lax.dynamic_slice(new_place[:, 0], (half * near_count,), (near_count,))
    gate_row = gate_prob.reshape(1, -1)
    own, other = half.reshape(1), (1 - half).reshape(1)
    me_one, plane_one = me.reshape(1), plane.reshape(1)

    mine = master.astype(jnp.bfloat16)
    lows, highs = along_line(mine, line, wide)
    wanted = lax.dynamic_slice(old, (plane * peers,), (peers,))[
        me ^ jnp.arange(peers, dtype=jnp.int32)
    ]
    sets = {"near": ([(mine,)], [0]), "mid": ([], []), "far": ([], [])}
    for r in range(1, line):
        blocks, offs = sets["near" if r == 1 else "far" if r == line - 1 else "mid"]
        if 2 * r < line:
            blocks += [(lows[r - 1],), (highs[r - 1],)]
            offs += [-r, r]
        else:
            blocks.append((lows[r - 1], highs[r - 1], r))
            offs.append(jnp.where(plane >= r, -r, r))

    def table(offs):
        at = plane + jnp.stack([jnp.asarray(o, jnp.int32) for o in offs])
        valid = (at >= 0) & (at < line)
        return jnp.clip(at, 0, line - 1), valid.astype(jnp.int32)

    def back_part(name, so_far, last=None):
        blocks, offs = sets[name]
        parts = among_peers(picked(plane_one, wanted, blocks, name == "far"), peers, devices)
        return back(me_one, *table(offs), cotangent, parts, wide, slot_count, so_far, last)

    grads = slot_grads(row_counts, rows_in, cotangent, gate_row, group_count)
    arrived = exchange(grads.reshape(-1, part_rows, part_cols), ALL)
    so_far = back_part("near", None)
    new_master, new_first, new_second, fresh, send = update(
        old, new, arrived, master, moment_one, moment_two
    )
    weight = exchange(send, HALF).reshape(inner, ff, part_cols)
    fresh = across(fresh)
    so_far = back_part("mid", so_far)
    next_out = next_rows(own, rows_next, weight)
    picks = half_picked(new, fresh)
    weight = exchange(picks, HALF).reshape(inner, ff, part_cols)
    input_grad, gate_grad = back_part("far", so_far, (row_counts, rows_in, gate_row))
    next_out = next_rows(other, rows_next, weight, next_out)
    return input_grad, gate_grad.reshape(-1), new_master, new_first, new_second, next_out


def solution(mesh):
    groups, slot_count = mesh.devices.shape
    mesh = Mesh(mesh.devices.reshape(2, groups // 2, slot_count), ALL)
    rows = P(ALL, None)
    row = P(ALL)
    state = P(None, "slot", ("half", "inner"))
    return jax.shard_map(
        shards,
        mesh=mesh,
        in_specs=(rows, rows, row, row, P(), P(), rows, state, state, state),
        out_specs=(rows, row, state, state, state, rows),
        check_vma=False,
    )
```

```python
import functools

import jax
import jax.numpy as jnp
from jax import lax
from jax.experimental import pallas as pl
from jax.experimental.pallas import tpu as pltpu
from jax.sharding import Mesh
from jax.sharding import PartitionSpec as P

beta_one = 0.9
beta_two = 0.999
adam_eps = 1e-08
learn_rate = 0.006
fix_one = 0.9999734386011124
fix_two = 0.0952078528862904

WHOLE_VMEM = 67_000_000

LINE = ("half", "inner")
HALF = ("inner", "slot")
ALL = ("half", "inner", "slot")


def column_of(row):
    return jnp.transpose(jnp.broadcast_to(row, (8, row.shape[1])))[:, :1]


def slot_grad_kernel(half_ref, count_ref, rows_ref, cot_ref, gate_ref, out_ref, turned):
    rows = rows_ref.shape[0]
    live = lax.broadcasted_iota(jnp.int32, (rows, 1), 0) < count_ref[0]

    @pl.when(pl.program_id(0) == 0)
    def _():
        kept = jnp.where(live, rows_ref[...].astype(jnp.float32), 0.0)
        turned[...] = jnp.transpose(kept).astype(jnp.bfloat16)

    scaled = column_of(gate_ref[...]) * cot_ref[...].astype(jnp.float32)
    scaled = jnp.where(live, scaled, 0.0).astype(jnp.bfloat16)
    cols = out_ref.shape[2]
    for i in range(out_ref.shape[0]):
        out_ref[i] = jnp.dot(
            turned[...],
            scaled[:, i * cols : (i + 1) * cols],
            preferred_element_type=jnp.float32,
        ).astype(jnp.bfloat16)


def slot_grads(half, row_counts, rows_in, cotangent, gate_row, inner):
    rows, ff = rows_in.shape
    cols = cotangent.shape[1] // (2 * inner)
    pair = inner // 2
    return pl.pallas_call(
        slot_grad_kernel,
        name="slot_grads",
        out_shape=jax.ShapeDtypeStruct((inner, ff, cols), jnp.bfloat16),
        grid_spec=pltpu.PrefetchScalarGridSpec(
            num_scalar_prefetch=2,
            grid=(pair,),
            in_specs=[
                pl.BlockSpec((rows, ff), lambda g, h, c: (0, 0)),
                pl.BlockSpec((rows, 2 * cols), lambda g, h, c: (0, h[0] * pair + g)),
                pl.BlockSpec((1, rows), lambda g, h, c: (0, 0)),
            ],
            out_specs=pl.BlockSpec((2, ff, cols), lambda g, h, c: (g, 0, 0)),
            scratch_shapes=[pltpu.VMEM((ff, rows), jnp.bfloat16)],
        ),
        compiler_params=pltpu.CompilerParams(
            dimension_semantics=("arbitrary",), vmem_limit_bytes=WHOLE_VMEM
        ),
    )(half, row_counts, rows_in, cotangent, gate_row)


def add_slots(place_ref, grads_ref, total):
    def add(s, _):
        e = place_ref[s]
        total[e] = total[e] + grads_ref[s].astype(jnp.float32)
        return 0

    lax.fori_loop(0, grads_ref.shape[0], add, 0, unroll=8)


def rows_step(rows):
    return max(d for d in (16, 32, 48) if rows % d == 0)


def sum_kernel(place_ref, grads_ref, out_ref, total):
    total[...] = jnp.zeros_like(total)
    add_slots(place_ref, grads_ref, total)
    out_ref[...] = total[...].astype(jnp.bfloat16)


def expert_sums(place, grads, experts):
    slots, rows, cols = grads.shape
    step = rows_step(rows)
    return pl.pallas_call(
        sum_kernel,
        name="expert_sums",
        out_shape=jax.ShapeDtypeStruct((experts, rows, cols), jnp.bfloat16),
        grid_spec=pltpu.PrefetchScalarGridSpec(
            num_scalar_prefetch=1,
            grid=(rows // step,),
            in_specs=[pl.BlockSpec((slots, step, cols), lambda i, a: (0, i, 0))],
            out_specs=pl.BlockSpec((experts, step, cols), lambda i, a: (0, i, 0)),
            scratch_shapes=[pltpu.VMEM((experts, step, cols), jnp.float32)],
        ),
        compiler_params=pltpu.CompilerParams(
            dimension_semantics=("arbitrary",), vmem_limit_bytes=WHOLE_VMEM
        ),
    )(place, grads)


def update_kernel(
    old_ref, new_ref, grads_ref, sums_ref, master_ref, one_ref, two_ref,
    master_out, one_out, two_out, fresh_ref, send_ref, total,
):
    total[...] = sums_ref[...].astype(jnp.float32)
    add_slots(old_ref, grads_ref, total)
    grad = total[...]
    first = beta_one * one_ref[...].astype(jnp.float32) + (1.0 - beta_one) * grad
    second = beta_two * two_ref[...].astype(jnp.float32) + (1.0 - beta_two) * grad * grad
    master = master_ref[...] - (learn_rate / fix_one) * first / (
        jnp.sqrt(second * (1.0 / fix_two)) + adam_eps
    )
    master_out[...] = master
    one_out[...] = first.astype(jnp.bfloat16)
    two_out[...] = second.astype(jnp.bfloat16)
    fresh_ref[...] = master.astype(jnp.bfloat16)

    def pick(s, _):
        send_ref[s] = fresh_ref[new_ref[s]]
        return 0

    lax.fori_loop(0, send_ref.shape[0], pick, 0, unroll=8)


def update(old, new, grads, sums, master, one, two):
    slots, rows, cols = grads.shape
    experts = master.shape[0]
    step = rows_step(rows)
    state = pl.BlockSpec((experts, step, cols), lambda i, a, b: (0, i, 0))
    wide = pl.BlockSpec((slots, step, cols), lambda i, a, b: (0, i, 0))
    near = pl.BlockSpec((new.shape[0], step, cols), lambda i, a, b: (0, i, 0))
    return pl.pallas_call(
        update_kernel,
        name="update",
        out_shape=(
            jax.ShapeDtypeStruct(master.shape, jnp.float32),
            jax.ShapeDtypeStruct(master.shape, jnp.bfloat16),
            jax.ShapeDtypeStruct(master.shape, jnp.bfloat16),
            jax.ShapeDtypeStruct(master.shape, jnp.bfloat16),
            jax.ShapeDtypeStruct(new.shape + (rows, cols), jnp.bfloat16),
        ),
        grid_spec=pltpu.PrefetchScalarGridSpec(
            num_scalar_prefetch=2,
            grid=(rows // step,),
            in_specs=[wide, state, state, state, state],
            out_specs=[state, state, state, state, near],
            scratch_shapes=[pltpu.VMEM((experts, step, cols), jnp.float32)],
        ),
        compiler_params=pltpu.CompilerParams(
            dimension_semantics=("arbitrary",), vmem_limit_bytes=WHOLE_VMEM
        ),
    )(old, new, grads, sums, master, one, two)


def next_kernel(half_ref, rows_ref, weight_ref, *rest):
    out_ref = rest[-1]
    cols = weight_ref.shape[2]
    for i in range(2):
        out_ref[:, i * cols : (i + 1) * cols] = jnp.dot(
            rows_ref[...],
            weight_ref[2 * pl.program_id(0) + i],
            preferred_element_type=jnp.float32,
        ).astype(jnp.bfloat16)


def next_rows(half, rows_next, weight, so_far=None):
    inner, _, cols = weight.shape
    rows = rows_next.shape[0]
    pair = inner // 2
    more = () if so_far is None else (so_far,)
    return pl.pallas_call(
        next_kernel,
        name="next_rows",
        out_shape=jax.ShapeDtypeStruct((rows, 2 * inner * cols), jnp.bfloat16),
        grid_spec=pltpu.PrefetchScalarGridSpec(
            num_scalar_prefetch=1,
            grid=(pair,),
            in_specs=[pl.BlockSpec(memory_space=pltpu.VMEM)] * 2
            + [pl.BlockSpec(memory_space=pl.ANY)] * len(more),
            out_specs=pl.BlockSpec((rows, 2 * cols), lambda g, h: (0, h[0] * pair + g)),
        ),
        input_output_aliases={3: 0} if more else {},
        compiler_params=pltpu.CompilerParams(
            dimension_semantics=("arbitrary",), vmem_limit_bytes=WHOLE_VMEM
        ),
    )(half, rows_next, weight, *more)


def half_pick_kernel(wanted_ref, block_ref, out_ref):
    def pick(p, _):
        out_ref[p] = block_ref[wanted_ref[p]]
        return 0

    lax.fori_loop(0, out_ref.shape[0], pick, 0, unroll=4)


def half_picked(wanted, block):
    return pl.pallas_call(
        half_pick_kernel,
        name="half_picked",
        out_shape=jax.ShapeDtypeStruct(wanted.shape + block.shape[1:], jnp.bfloat16),
        in_specs=[
            pl.BlockSpec(memory_space=pltpu.SMEM),
            pl.BlockSpec(memory_space=pltpu.VMEM),
        ],
        out_specs=pl.BlockSpec(memory_space=pltpu.VMEM),
        compiler_params=pltpu.CompilerParams(vmem_limit_bytes=WHOLE_VMEM),
    )(wanted, block)


def along_line(mine, line, wide):
    low, high, lows, highs = mine, mine, [], []
    for turn in range(line - 1):
        ups = [(g, g + wide) for g in range(turn * wide, (line - 1) * wide)]
        downs = [(g + wide, g) for g in range((line - 1 - turn) * wide)]
        low = lax.ppermute(low, LINE, ups)
        high = lax.ppermute(high, LINE, downs)
        lows.append(low)
        highs.append(high)
    return lows, highs


def pick_kernel(pairs, plane_ref, wanted_ref, *rest):
    count = sum(2 if p else 1 for p in pairs)
    blocks, outs, sems = rest[:count], rest[count:-1], rest[-1]
    for j, out in enumerate(outs):
        at = 0
        for i, reach in enumerate(pairs):
            if not reach:
                pltpu.make_async_copy(
                    blocks[at].at[wanted_ref[j]], out.at[i], sems.at[j]
                ).start()
                at += 1
                continue
            for side in range(2):

                @pl.when((plane_ref[0] >= reach) == (side == 0))
                def _(block=blocks[at + side], out=out, i=i, j=j):
                    pltpu.make_async_copy(
                        block.at[wanted_ref[j]], out.at[i], sems.at[j]
                    ).start()

            at += 2
    for j, out in enumerate(outs):
        pltpu.make_async_copy(out, out, sems.at[j]).wait()


def picked(plane, wanted, entries, held=False):
    pairs = [entry[2] if len(entry) == 3 else 0 for entry in entries]
    blocks = [block for entry in entries for block in entry[:2]]
    piece = (len(entries),) + blocks[0].shape[1:]
    peers = wanted.shape[0]
    return pl.pallas_call(
        functools.partial(held_pick_kernel if held else pick_kernel, pairs),
        name="picked",
        out_shape=[jax.ShapeDtypeStruct(piece, jnp.bfloat16)] * peers,
        in_specs=[pl.BlockSpec(memory_space=pltpu.SMEM)] * 2
        + [pl.BlockSpec(memory_space=pltpu.VMEM if held else pl.ANY)] * len(blocks),
        out_specs=[pl.BlockSpec(memory_space=pltpu.VMEM)] * peers,
        scratch_shapes=[] if held else [pltpu.SemaphoreType.DMA((peers,))],
        compiler_params=pltpu.CompilerParams(vmem_limit_bytes=WHOLE_VMEM),
    )(plane, wanted, *blocks)


def held_pick_kernel(pairs, plane_ref, wanted_ref, *rest):
    count = sum(2 if p else 1 for p in pairs)
    blocks, outs = rest[:count], rest[count:]
    at = 0
    for i, reach in enumerate(pairs):
        if not reach:
            for j, out in enumerate(outs):
                out[i] = blocks[at][wanted_ref[j]]
            at += 1
            continue
        for side in range(2):

            @pl.when((plane_ref[0] >= reach) == (side == 0))
            def _(block=blocks[at + side], i=i):
                for j, out in enumerate(outs):
                    out[i] = block[wanted_ref[j]]

        at += 2


def among_peers(picks, peers, devices):
    parts = [picks[0]]
    for j in range(1, peers):
        pairs = [(p, p - p % peers + (p % peers ^ j)) for p in range(devices)]
        parts.append(lax.ppermute(picks[j], ALL, pairs))
    return parts


def back_kernel(wide, peers, slot_count, last, me_ref, plane_ref, valid_ref, *rest):
    parts, rest = rest[:peers], rest[peers:]
    cot_ref, rest = rest[0], rest[1:]
    if last:
        count_ref, rows_ref, gate_ref, so_far, grad_ref, gate_out, total, held, sems = rest
    elif len(rest) == 4:
        so_far, total, held, sems = rest
    else:
        so_far, (total, held, sems) = None, rest
    i = pl.program_id(0)

    @pl.when(i == 0)
    def _():
        copies = [pltpu.make_async_copy(part, held.at[j], sems.at[j]) for j, part in enumerate(parts)]
        for copy in copies:
            copy.start()
        total[...] = jnp.zeros_like(total) if so_far is None else so_far[...]
        for copy in copies:
            copy.wait()

    @pl.when(valid_ref[i // wide] == 1)
    def _():
        weight = jnp.concatenate(
            [
                held[((i % wide) * slot_count + k) ^ me_ref[0], i // wide]
                for k in range(slot_count)
            ],
            axis=0,
        )
        total[...] += lax.dot_general(
            cot_ref[...], weight, (((1,), (1,)), ((), ())), preferred_element_type=jnp.float32
        )

    if last:

        @pl.when(i == pl.num_programs(0) - 1)
        def _():
            rows = rows_ref.shape[0]
            live = lax.broadcasted_iota(jnp.int32, (rows, 1), 0) < count_ref[0]
            back = jnp.where(live, total[...], 0.0)
            grad_ref[...] = (column_of(gate_ref[...]) * back).astype(jnp.bfloat16)
            summed = jnp.sum(rows_ref[...].astype(jnp.float32) * back, axis=1, keepdims=True)
            gate_out[...] = jnp.transpose(jnp.broadcast_to(summed, (rows, 128)))[:1]


def back(me, planes, valid, cotangent, parts, wide, slot_count, so_far=None, last=None):
    peers = len(parts)
    entries, part_rows, cols = parts[0].shape
    rows, ff = cotangent.shape[0], slot_count * part_rows
    whole = pl.BlockSpec((rows, ff), lambda i, *_: (0, 0))
    row = pl.BlockSpec((1, rows), lambda i, *_: (0, 0))

    def taken(i, m, plane, *_):
        return (0, plane[i // wide] * wide + i % wide)

    total = jax.ShapeDtypeStruct((rows, ff), jnp.float32)
    specs = [pl.BlockSpec(memory_space=pl.ANY)] * peers + [pl.BlockSpec((rows, cols), taken)]
    scratch = [
        pltpu.VMEM((peers, entries, part_rows, cols), jnp.bfloat16),
        pltpu.SemaphoreType.DMA((peers,)),
    ]
    more = ()
    if last is not None:
        specs += [pl.BlockSpec(memory_space=pltpu.SMEM), whole, row]
        more = last
        total = (
            jax.ShapeDtypeStruct((rows, ff), jnp.bfloat16),
            jax.ShapeDtypeStruct((1, rows), jnp.float32),
        )
        scratch = [pltpu.VMEM((rows, ff), jnp.float32)] + scratch
    if so_far is not None:
        specs.append(whole)
        more += (so_far,)
    return pl.pallas_call(
        functools.partial(back_kernel, wide, peers, slot_count, last is not None),
        name="back",
        out_shape=total,
        grid_spec=pltpu.PrefetchScalarGridSpec(
            num_scalar_prefetch=3,
            grid=(entries * wide,),
            in_specs=specs,
            out_specs=whole if last is None else [whole, row],
            scratch_shapes=scratch,
        ),
        compiler_params=pltpu.CompilerParams(
            dimension_semantics=("arbitrary",), vmem_limit_bytes=WHOLE_VMEM
        ),
    )(me, planes, valid, *parts, cotangent, *more)


def exchange(blocks):
    return lax.all_to_all(blocks, HALF, split_axis=0, concat_axis=0, tiled=True)


def across(block):
    return lax.ppermute(block, "half", [(0, 1), (1, 0)])


def shards(
    rows_in, cotangent, gate_prob, row_counts, old_place, new_place, rows_next,
    master, moment_one, moment_two,
):
    inner, slot_count = lax.axis_size("inner"), lax.axis_size("slot")
    group_count, near_count = 2 * inner, inner * slot_count
    devices = group_count * slot_count
    experts, part_rows, part_cols = master.shape
    ff = slot_count * part_rows
    wide = 2
    line = group_count // wide
    peers = wide * slot_count
    half = lax.axis_index("half")
    g_own, k_own = half * inner + lax.axis_index("inner"), lax.axis_index("slot")
    plane = g_own // wide
    me = (g_own % wide) * slot_count + k_own
    old = old_place[:, 0]
    old_near = lax.dynamic_slice(old, (half * near_count,), (near_count,))
    new = lax.dynamic_slice(new_place[:, 0], (half * near_count,), (near_count,))
    gate_row = gate_prob.reshape(1, -1)
    own, other = half.reshape(1), (1 - half).reshape(1)
    me_one, plane_one = me.reshape(1), plane.reshape(1)

    mine = master.astype(jnp.bfloat16)
    lows, highs = along_line(mine, line, wide)
    wanted = lax.dynamic_slice(old, (plane * peers,), (peers,))[
        me ^ jnp.arange(peers, dtype=jnp.int32)
    ]
    sets = {"near": ([(mine,)], [0]), "mid": ([], []), "far": ([], [])}
    for r in range(1, line):
        blocks, offs = sets["near" if r == 1 else "far" if r == line - 1 else "mid"]
        if 2 * r < line:
            blocks += [(lows[r - 1],), (highs[r - 1],)]
            offs += [-r, r]
        else:
            blocks.append((lows[r - 1], highs[r - 1], r))
            offs.append(jnp.where(plane >= r, -r, r))

    def table(offs):
        at = plane + jnp.stack([jnp.asarray(o, jnp.int32) for o in offs])
        valid = (at >= 0) & (at < line)
        return jnp.clip(at, 0, line - 1), valid.astype(jnp.int32)

    def back_part(name, so_far, last=None):
        blocks, offs = sets[name]
        parts = among_peers(picked(plane_one, wanted, blocks, name == "far"), peers, devices)
        return back(me_one, *table(offs), cotangent, parts, wide, slot_count, so_far, last)

    def blocks_of(grads):
        return grads.reshape(near_count, part_rows, part_cols)

    grads = slot_grads(other, row_counts, rows_in, cotangent, gate_row, inner)
    arrived = exchange(blocks_of(grads))
    grads = slot_grads(own, row_counts, rows_in, cotangent, gate_row, inner)
    sums = expert_sums(old_near, arrived, experts)
    sums = across(sums)
    arrived = exchange(blocks_of(grads))
    so_far = back_part("near", None)
    new_master, new_first, new_second, fresh, send = update(
        old_near, new, arrived, sums, master, moment_one, moment_two
    )
    weight = exchange(send).reshape(inner, ff, part_cols)
    fresh = across(fresh)
    so_far = back_part("mid", so_far)
    next_out = next_rows(own, rows_next, weight)
    picks = half_picked(new, fresh)
    weight = exchange(picks).reshape(inner, ff, part_cols)
    input_grad, gate_grad = back_part("far", so_far, (row_counts, rows_in, gate_row))
    next_out = next_rows(other, rows_next, weight, next_out)
    return input_grad, gate_grad.reshape(-1), new_master, new_first, new_second, next_out


def solution(mesh):
    groups, slot_count = mesh.devices.shape
    mesh = Mesh(mesh.devices.reshape(2, groups // 2, slot_count), ALL)
    rows = P(ALL, None)
    row = P(ALL)
    state = P(None, "slot", ("half", "inner"))
    return jax.shard_map(
        shards,
        mesh=mesh,
        in_specs=(rows, rows, row, row, P(), P(), rows, state, state, state),
        out_specs=(rows, row, state, state, state, rows),
        check_vma=False,
    )
```

```python
import functools

import jax
import jax.numpy as jnp
from jax import lax
from jax.experimental import pallas as pl
from jax.experimental.pallas import tpu as pltpu
from jax.sharding import Mesh
from jax.sharding import PartitionSpec as P

beta_one = 0.9
beta_two = 0.999
adam_eps = 1e-08
learn_rate = 0.006
fix_one = 0.9999734386011124
fix_two = 0.0952078528862904

WHOLE_VMEM = 67_000_000

LINE = ("half", "inner")
HALF = ("inner", "slot")
ALL = ("half", "inner", "slot")


def column_of(row):
    return jnp.transpose(jnp.broadcast_to(row, (8, row.shape[1])))[:, :1]


def slot_grad_kernel(half_ref, count_ref, rows_ref, cot_ref, gate_ref, out_ref, turned):
    rows = rows_ref.shape[0]
    live = lax.broadcasted_iota(jnp.int32, (rows, 1), 0) < count_ref[0]

    @pl.when(pl.program_id(0) == 0)
    def _():
        kept = jnp.where(live, rows_ref[...].astype(jnp.float32), 0.0)
        turned[...] = jnp.transpose(kept).astype(jnp.bfloat16)

    scaled = column_of(gate_ref[...]) * cot_ref[...].astype(jnp.float32)
    scaled = jnp.where(live, scaled, 0.0).astype(jnp.bfloat16)
    cols = out_ref.shape[2]
    for i in range(out_ref.shape[0]):
        out_ref[i] = jnp.dot(
            turned[...],
            scaled[:, i * cols : (i + 1) * cols],
            preferred_element_type=jnp.float32,
        ).astype(jnp.bfloat16)


def slot_grads(half, row_counts, rows_in, cotangent, gate_row, inner):
    rows, ff = rows_in.shape
    cols = cotangent.shape[1] // (2 * inner)
    pair = inner // 2
    return pl.pallas_call(
        slot_grad_kernel,
        name="slot_grads",
        out_shape=jax.ShapeDtypeStruct((inner, ff, cols), jnp.bfloat16),
        grid_spec=pltpu.PrefetchScalarGridSpec(
            num_scalar_prefetch=2,
            grid=(pair,),
            in_specs=[
                pl.BlockSpec((rows, ff), lambda g, h, c: (0, 0)),
                pl.BlockSpec((rows, 2 * cols), lambda g, h, c: (0, h[0] * pair + g)),
                pl.BlockSpec((1, rows), lambda g, h, c: (0, 0)),
            ],
            out_specs=pl.BlockSpec((2, ff, cols), lambda g, h, c: (g, 0, 0)),
            scratch_shapes=[pltpu.VMEM((ff, rows), jnp.bfloat16)],
        ),
        compiler_params=pltpu.CompilerParams(
            dimension_semantics=("arbitrary",), vmem_limit_bytes=WHOLE_VMEM
        ),
    )(half, row_counts, rows_in, cotangent, gate_row)


def add_slots(place_ref, grads_ref, total):
    def add(s, _):
        e = place_ref[s]
        total[e] = total[e] + grads_ref[s].astype(jnp.float32)
        return 0

    lax.fori_loop(0, grads_ref.shape[0], add, 0, unroll=8)


def rows_step(rows, most):
    return max(d for d in (16, 32, 48, 96) if d <= most and rows % d == 0)


def sum_kernel(place_ref, grads_ref, out_ref, total):
    total[...] = jnp.zeros_like(total)
    add_slots(place_ref, grads_ref, total)
    out_ref[...] = total[...].astype(jnp.bfloat16)


def expert_sums(place, grads, experts):
    slots, rows, cols = grads.shape
    step = rows_step(rows, 48)
    return pl.pallas_call(
        sum_kernel,
        name="expert_sums",
        out_shape=jax.ShapeDtypeStruct((experts, rows, cols), jnp.bfloat16),
        grid_spec=pltpu.PrefetchScalarGridSpec(
            num_scalar_prefetch=1,
            grid=(rows // step,),
            in_specs=[pl.BlockSpec((slots, step, cols), lambda i, a: (0, i, 0))],
            out_specs=pl.BlockSpec((experts, step, cols), lambda i, a: (0, i, 0)),
            scratch_shapes=[pltpu.VMEM((experts, step, cols), jnp.float32)],
        ),
        compiler_params=pltpu.CompilerParams(
            dimension_semantics=("arbitrary",), vmem_limit_bytes=WHOLE_VMEM
        ),
    )(place, grads)


def update_kernel(
    old_ref, new_ref, grads_ref, sums_ref, master_ref, one_ref, two_ref,
    master_out, one_out, two_out, fresh_ref, send_ref, total,
):
    total[...] = sums_ref[...].astype(jnp.float32)
    add_slots(old_ref, grads_ref, total)
    grad = total[...]
    first = beta_one * one_ref[...].astype(jnp.float32) + (1.0 - beta_one) * grad
    second = beta_two * two_ref[...].astype(jnp.float32) + (1.0 - beta_two) * grad * grad
    master = master_ref[...] - (learn_rate / fix_one) * first / (
        jnp.sqrt(second * (1.0 / fix_two)) + adam_eps
    )
    master_out[...] = master
    one_out[...] = first.astype(jnp.bfloat16)
    two_out[...] = second.astype(jnp.bfloat16)
    fresh_ref[...] = master.astype(jnp.bfloat16)

    def pick(s, _):
        send_ref[s] = fresh_ref[new_ref[s]]
        return 0

    lax.fori_loop(0, send_ref.shape[0], pick, 0, unroll=8)


def update(old, new, grads, sums, master, one, two):
    slots, rows, cols = grads.shape
    experts = master.shape[0]
    step = rows_step(rows, 96)
    state = pl.BlockSpec((experts, step, cols), lambda i, a, b: (0, i, 0))
    wide = pl.BlockSpec((slots, step, cols), lambda i, a, b: (0, i, 0))
    near = pl.BlockSpec((new.shape[0], step, cols), lambda i, a, b: (0, i, 0))
    return pl.pallas_call(
        update_kernel,
        name="update",
        out_shape=(
            jax.ShapeDtypeStruct(master.shape, jnp.float32),
            jax.ShapeDtypeStruct(master.shape, jnp.bfloat16),
            jax.ShapeDtypeStruct(master.shape, jnp.bfloat16),
            jax.ShapeDtypeStruct(master.shape, jnp.bfloat16),
            jax.ShapeDtypeStruct(new.shape + (rows, cols), jnp.bfloat16),
        ),
        grid_spec=pltpu.PrefetchScalarGridSpec(
            num_scalar_prefetch=2,
            grid=(rows // step,),
            in_specs=[wide, state, state, state, state],
            out_specs=[state, state, state, state, near],
            scratch_shapes=[pltpu.VMEM((experts, step, cols), jnp.float32)],
        ),
        compiler_params=pltpu.CompilerParams(
            dimension_semantics=("arbitrary",), vmem_limit_bytes=WHOLE_VMEM
        ),
    )(old, new, grads, sums, master, one, two)


def next_kernel(half_ref, rows_ref, weight_ref, *rest):
    out_ref = rest[-1]
    cols = weight_ref.shape[2]
    for i in range(2):
        out_ref[:, i * cols : (i + 1) * cols] = jnp.dot(
            rows_ref[...],
            weight_ref[i],
            preferred_element_type=jnp.float32,
        ).astype(jnp.bfloat16)


def next_rows(half, rows_next, weight, so_far=None):
    inner, ff, cols = weight.shape
    rows = rows_next.shape[0]
    pair = inner // 2
    more = () if so_far is None else (so_far,)
    return pl.pallas_call(
        next_kernel,
        name="next_rows",
        out_shape=jax.ShapeDtypeStruct((rows, 2 * inner * cols), jnp.bfloat16),
        grid_spec=pltpu.PrefetchScalarGridSpec(
            num_scalar_prefetch=1,
            grid=(pair,),
            in_specs=[
                pl.BlockSpec(memory_space=pltpu.VMEM),
                pl.BlockSpec((2, ff, cols), lambda g, h: (g, 0, 0)),
            ]
            + [pl.BlockSpec(memory_space=pl.ANY)] * len(more),
            out_specs=pl.BlockSpec((rows, 2 * cols), lambda g, h: (0, h[0] * pair + g)),
        ),
        input_output_aliases={3: 0} if more else {},
        compiler_params=pltpu.CompilerParams(
            dimension_semantics=("arbitrary",), vmem_limit_bytes=WHOLE_VMEM
        ),
    )(half, rows_next, weight, *more)


def half_pick_kernel(wanted_ref, block_ref, out_ref):
    def pick(p, _):
        out_ref[p] = block_ref[wanted_ref[p]]
        return 0

    lax.fori_loop(0, out_ref.shape[0], pick, 0, unroll=4)


def half_picked(wanted, block):
    return pl.pallas_call(
        half_pick_kernel,
        name="half_picked",
        out_shape=jax.ShapeDtypeStruct(wanted.shape + block.shape[1:], jnp.bfloat16),
        in_specs=[
            pl.BlockSpec(memory_space=pltpu.SMEM),
            pl.BlockSpec(memory_space=pltpu.VMEM),
        ],
        out_specs=pl.BlockSpec(memory_space=pltpu.VMEM),
        compiler_params=pltpu.CompilerParams(vmem_limit_bytes=WHOLE_VMEM),
    )(wanted, block)


def along_line(mine, line, wide):
    low, high, lows, highs = mine, mine, [], []
    for turn in range(line - 1):
        ups = [(g, g + wide) for g in range(turn * wide, (line - 1) * wide)]
        downs = [(g + wide, g) for g in range((line - 1 - turn) * wide)]
        low = lax.ppermute(low, LINE, ups)
        high = lax.ppermute(high, LINE, downs)
        lows.append(low)
        highs.append(high)
    return lows, highs


def pick_kernel(pairs, plane_ref, wanted_ref, *rest):
    count = sum(2 if p else 1 for p in pairs)
    blocks, outs, sems = rest[:count], rest[count:-1], rest[-1]
    for j, out in enumerate(outs):
        at = 0
        for i, reach in enumerate(pairs):
            if not reach:
                pltpu.make_async_copy(
                    blocks[at].at[wanted_ref[j]], out.at[i], sems.at[j]
                ).start()
                at += 1
                continue
            for side in range(2):

                @pl.when((plane_ref[0] >= reach) == (side == 0))
                def _(block=blocks[at + side], out=out, i=i, j=j):
                    pltpu.make_async_copy(
                        block.at[wanted_ref[j]], out.at[i], sems.at[j]
                    ).start()

            at += 2
    for j, out in enumerate(outs):
        pltpu.make_async_copy(out, out, sems.at[j]).wait()


def picked(plane, wanted, entries, held=False):
    pairs = [entry[2] if len(entry) == 3 else 0 for entry in entries]
    blocks = [block for entry in entries for block in entry[:2]]
    piece = (len(entries),) + blocks[0].shape[1:]
    peers = wanted.shape[0]
    return pl.pallas_call(
        functools.partial(held_pick_kernel if held else pick_kernel, pairs),
        name="picked",
        out_shape=[jax.ShapeDtypeStruct(piece, jnp.bfloat16)] * peers,
        in_specs=[pl.BlockSpec(memory_space=pltpu.SMEM)] * 2
        + [pl.BlockSpec(memory_space=pltpu.VMEM if held else pl.ANY)] * len(blocks),
        out_specs=[pl.BlockSpec(memory_space=pltpu.VMEM)] * peers,
        scratch_shapes=[] if held else [pltpu.SemaphoreType.DMA((peers,))],
        compiler_params=pltpu.CompilerParams(vmem_limit_bytes=WHOLE_VMEM),
    )(plane, wanted, *blocks)


def held_pick_kernel(pairs, plane_ref, wanted_ref, *rest):
    count = sum(2 if p else 1 for p in pairs)
    blocks, outs = rest[:count], rest[count:]
    at = 0
    for i, reach in enumerate(pairs):
        if not reach:
            for j, out in enumerate(outs):
                out[i] = blocks[at][wanted_ref[j]]
            at += 1
            continue
        for side in range(2):

            @pl.when((plane_ref[0] >= reach) == (side == 0))
            def _(block=blocks[at + side], i=i):
                for j, out in enumerate(outs):
                    out[i] = block[wanted_ref[j]]

        at += 2


def among_peers(picks, peers, devices):
    parts = [picks[0]]
    for j in range(1, peers):
        pairs = [(p, p - p % peers + (p % peers ^ j)) for p in range(devices)]
        parts.append(lax.ppermute(picks[j], ALL, pairs))
    return parts


def back_kernel(wide, peers, slot_count, last, me_ref, plane_ref, valid_ref, *rest):
    parts, rest = rest[:peers], rest[peers:]
    cot_ref, rest = rest[0], rest[1:]
    if last:
        count_ref, rows_ref, gate_ref, so_far, grad_ref, gate_out, total, held, sems = rest
    elif len(rest) == 4:
        so_far, total, held, sems = rest
    else:
        so_far, (total, held, sems) = None, rest
    i = pl.program_id(0)

    @pl.when(i == 0)
    def _():
        copies = [pltpu.make_async_copy(part, held.at[j], sems.at[j]) for j, part in enumerate(parts)]
        for copy in copies:
            copy.start()
        total[...] = jnp.zeros_like(total) if so_far is None else so_far[...]
        for copy in copies:
            copy.wait()

    @pl.when(valid_ref[i // wide] == 1)
    def _():
        weight = jnp.concatenate(
            [
                held[((i % wide) * slot_count + k) ^ me_ref[0], i // wide]
                for k in range(slot_count)
            ],
            axis=0,
        )
        total[...] += lax.dot_general(
            cot_ref[...], weight, (((1,), (1,)), ((), ())), preferred_element_type=jnp.float32
        )

    if last:

        @pl.when(i == pl.num_programs(0) - 1)
        def _():
            rows = rows_ref.shape[0]
            live = lax.broadcasted_iota(jnp.int32, (rows, 1), 0) < count_ref[0]
            back = jnp.where(live, total[...], 0.0)
            grad_ref[...] = (column_of(gate_ref[...]) * back).astype(jnp.bfloat16)
            summed = jnp.sum(rows_ref[...].astype(jnp.float32) * back, axis=1, keepdims=True)
            gate_out[...] = jnp.transpose(jnp.broadcast_to(summed, (rows, 128)))[:1]


def back(me, planes, valid, cotangent, parts, wide, slot_count, so_far=None, last=None):
    peers = len(parts)
    entries, part_rows, cols = parts[0].shape
    rows, ff = cotangent.shape[0], slot_count * part_rows
    whole = pl.BlockSpec((rows, ff), lambda i, *_: (0, 0))
    row = pl.BlockSpec((1, rows), lambda i, *_: (0, 0))

    def taken(i, m, plane, *_):
        return (0, plane[i // wide] * wide + i % wide)

    total = jax.ShapeDtypeStruct((rows, ff), jnp.float32)
    specs = [pl.BlockSpec(memory_space=pl.ANY)] * peers + [pl.BlockSpec((rows, cols), taken)]
    scratch = [
        pltpu.VMEM((peers, entries, part_rows, cols), jnp.bfloat16),
        pltpu.SemaphoreType.DMA((peers,)),
    ]
    more = ()
    if last is not None:
        specs += [pl.BlockSpec(memory_space=pltpu.SMEM), whole, row]
        more = last
        total = (
            jax.ShapeDtypeStruct((rows, ff), jnp.bfloat16),
            jax.ShapeDtypeStruct((1, rows), jnp.float32),
        )
        scratch = [pltpu.VMEM((rows, ff), jnp.float32)] + scratch
    if so_far is not None:
        specs.append(whole)
        more += (so_far,)
    return pl.pallas_call(
        functools.partial(back_kernel, wide, peers, slot_count, last is not None),
        name="back",
        out_shape=total,
        grid_spec=pltpu.PrefetchScalarGridSpec(
            num_scalar_prefetch=3,
            grid=(entries * wide,),
            in_specs=specs,
            out_specs=whole if last is None else [whole, row],
            scratch_shapes=scratch,
        ),
        compiler_params=pltpu.CompilerParams(
            dimension_semantics=("arbitrary",), vmem_limit_bytes=WHOLE_VMEM
        ),
    )(me, planes, valid, *parts, cotangent, *more)


def exchange(blocks):
    return lax.all_to_all(blocks, HALF, split_axis=0, concat_axis=0, tiled=True)


def across(block):
    return lax.ppermute(block, "half", [(0, 1), (1, 0)])


def shards(
    rows_in, cotangent, gate_prob, row_counts, old_place, new_place, rows_next,
    master, moment_one, moment_two,
):
    inner, slot_count = lax.axis_size("inner"), lax.axis_size("slot")
    group_count, near_count = 2 * inner, inner * slot_count
    devices = group_count * slot_count
    experts, part_rows, part_cols = master.shape
    ff = slot_count * part_rows
    wide = 2
    line = group_count // wide
    peers = wide * slot_count
    half = lax.axis_index("half")
    g_own, k_own = half * inner + lax.axis_index("inner"), lax.axis_index("slot")
    plane = g_own // wide
    me = (g_own % wide) * slot_count + k_own
    old = old_place[:, 0]
    old_near = lax.dynamic_slice(old, (half * near_count,), (near_count,))
    new = lax.dynamic_slice(new_place[:, 0], (half * near_count,), (near_count,))
    gate_row = gate_prob.reshape(1, -1)
    own, other = half.reshape(1), (1 - half).reshape(1)
    me_one, plane_one = me.reshape(1), plane.reshape(1)

    mine = master.astype(jnp.bfloat16)
    lows, highs = along_line(mine, line, wide)
    wanted = lax.dynamic_slice(old, (plane * peers,), (peers,))[
        me ^ jnp.arange(peers, dtype=jnp.int32)
    ]
    sets = {"near": ([(mine,)], [0]), "mid": ([], []), "far": ([], [])}
    for r in range(1, line):
        blocks, offs = sets["near" if r == 1 else "far" if r == line - 1 else "mid"]
        if 2 * r < line:
            blocks += [(lows[r - 1],), (highs[r - 1],)]
            offs += [-r, r]
        else:
            blocks.append((lows[r - 1], highs[r - 1], r))
            offs.append(jnp.where(plane >= r, -r, r))

    def table(offs):
        at = plane + jnp.stack([jnp.asarray(o, jnp.int32) for o in offs])
        valid = (at >= 0) & (at < line)
        return jnp.clip(at, 0, line - 1), valid.astype(jnp.int32)

    def back_part(name, so_far, last=None):
        blocks, offs = sets[name]
        parts = among_peers(picked(plane_one, wanted, blocks, name == "far"), peers, devices)
        return back(me_one, *table(offs), cotangent, parts, wide, slot_count, so_far, last)

    def blocks_of(grads):
        return grads.reshape(near_count, part_rows, part_cols)

    grads = slot_grads(other, row_counts, rows_in, cotangent, gate_row, inner)
    arrived = exchange(blocks_of(grads))
    grads = slot_grads(own, row_counts, rows_in, cotangent, gate_row, inner)
    sums = expert_sums(old_near, arrived, experts)
    sums = across(sums)
    arrived = exchange(blocks_of(grads))
    so_far = back_part("near", None)
    new_master, new_first, new_second, fresh, send = update(
        old_near, new, arrived, sums, master, moment_one, moment_two
    )
    weight = exchange(send).reshape(inner, ff, part_cols)
    fresh = across(fresh)
    so_far = back_part("mid", so_far)
    next_out = next_rows(own, rows_next, weight)
    picks = half_picked(new, fresh)
    weight = exchange(picks).reshape(inner, ff, part_cols)
    input_grad, gate_grad = back_part("far", so_far, (row_counts, rows_in, gate_row))
    next_out = next_rows(other, rows_next, weight, next_out)
    return input_grad, gate_grad.reshape(-1), new_master, new_first, new_second, next_out


def solution(mesh):
    groups, slot_count = mesh.devices.shape
    mesh = Mesh(mesh.devices.reshape(2, groups // 2, slot_count), ALL)
    rows = P(ALL, None)
    row = P(ALL)
    state = P(None, "slot", ("half", "inner"))
    return jax.shard_map(
        shards,
        mesh=mesh,
        in_specs=(rows, rows, row, row, P(), P(), rows, state, state, state),
        out_specs=(rows, row, state, state, state, rows),
        check_vma=False,
    )
```
